256 devices in a mesh: cfg: 64 (over z, x_lo, y), lat: 4 (over x_hi, core).
Axes of the slice: x: 4 (x_hi: 2, x_lo: 2; x = x_hi * 2 + x_lo), y: 4, z: 8, core: 2. Of those that a mesh axis runs over, the one named last changes fastest.
Arguments:
- latent_mode: float32 [128, 1048576], P('cfg', 'lat'), may hold values from -6 to 6
- latent_var: float32 [128, 1048576], P('cfg', 'lat'), may hold values from 0.05 to 2
- config_weight: float32 [128], P('cfg'), may hold values from 0.05 to 20
- grid_offset: float32 [64], replicated, may hold values from -3 to 3
Outputs:
- marginal_density: float32 [64, 1048576], P(None, ('cfg', 'lat'))
- marginal_moments: float32 [2, 1048576], P(None, ('cfg', 'lat'))
The draws below stay inside these ranges and needn't reach their ends.
All inputs are finite; a program needn't handle non-finite values.
Results may differ from the reference program's by a relative error of at most 0.00002.
Values sent between devices are 32-bit elements; how exact they have to be, the bound alone decides.
No kernel may reach another device: no remote copies, remote signals or barrier semaphores. Data moves between devices by JAX's collectives and lax.ppermute only.
A program may use at most 64 MiB of HBM per device.

```python
import math
import jax
import jax.numpy as jnp
from jax import lax

G = 64
K = 128
NLAT = 1048576


def shard_levels(stream_key, dims, cuts, low, top_value):
    def one(dim, parts):
        steps = jax.random.uniform(jax.random.fold_in(jax.random.fold_in(stream_key, 6), dim), (parts,), jnp.float32, low / len(cuts), top_value / len(cuts))
        return jnp.repeat(jnp.exp(steps), dims[dim] // parts).reshape((-1,) + (1,) * (len(dims) - dim - 1))

    factor_of = one(*cuts[0])
    for cut in cuts[1:]:
        factor_of = factor_of * one(*cut)
    return factor_of


def scatter_about(own_key, dims, scale, limit, cuts=(), held_as=jnp.bfloat16):
    result = jax.random.normal(own_key, dims, jnp.float32) * scale
    if len(cuts) > 0:
        result = shard_levels(own_key, dims, cuts, -0.22, 0.18) * result
    return jnp.clip(result, min=-limit, max=limit).astype(held_as)


def setup_inputs(seed: int = 0) -> dict:
    key_of = jax.random.split(jax.random.key(seed), 5)
    latent_mode = scatter_about(key_of[0], (K, NLAT), 1.0, 6.0, ((0, 64), (1, 4)), jnp.float32)
    latent_var = jnp.clip(jnp.exp(math.log(2.0) - 3.6888794 * jax.random.uniform(key_of[1], (K, NLAT), jnp.float32) ** shard_levels(key_of[1], (K, NLAT), ((0, 64), (1, 4)), -0.2, 0.2)), 0.05, 2.0)
    config_weight = jnp.clip(jnp.exp(math.log(20.0) - 5.9914645 * jax.random.uniform(key_of[2], (K,), jnp.float32) ** shard_levels(key_of[2], (K,), ((0, 64),), -0.2, 0.2)), 0.05, 20.0)
    grid_offset = jnp.clip(jax.random.uniform(key_of[3], (G,), jnp.float32, -3.0, 3.0), -3.0, 3.0)
    return {"latent_mode": latent_mode, "latent_var": latent_var, "config_weight": config_weight, "grid_offset": grid_offset}


def mixture(mode_block, var_block, norm_weight, grid_offset):
    centre = lax.optimization_barrier(jnp.sum(norm_weight[:, None] * mode_block, axis=0))
    deviation = mode_block - centre[None, :]
    spread = jnp.sqrt(lax.optimization_barrier(jnp.sum(norm_weight[:, None] * (var_block + deviation * deviation), axis=0)))
    points = centre[None, :] + grid_offset[:, None] * spread[None, :]
    coefficient = norm_weight[:, None] / jnp.sqrt(6.283185307179586 * var_block)
    precision = 1.0 / var_block
    gap = points[None, :, :] - mode_block[:, None, :]
    terms = coefficient[:, None, :] * jnp.exp(-0.5 * gap * gap * precision[:, None, :])
    density = spread[None, :] * lax.optimization_barrier(jnp.sum(terms, axis=0))
    return (density, jnp.stack([centre, spread], axis=0))

def reference(latent_mode, latent_var, config_weight, grid_offset):
    norm_weight = config_weight / jnp.sum(config_weight)
    width = min(NLAT, 4096)
    count = NLAT // width
    modes_blocked = latent_mode.reshape(K, count, width).transpose(1, 0, 2)
    vars_blocked = latent_var.reshape(K, count, width).transpose(1, 0, 2)

    def one_block(pair):
        return mixture(pair[0], pair[1], norm_weight, grid_offset)
    density, moments = lax.map(one_block, (modes_blocked, vars_blocked))
    density = density.transpose(1, 0, 2).reshape(G, NLAT)
    moments = moments.transpose(1, 0, 2).reshape(2, NLAT)
    return (density, moments)
```

```python
import functools

import jax
import jax.numpy as jnp
from jax import lax
from jax.experimental import pallas as pl
from jax.experimental.pallas import tpu as pltpu
from jax.sharding import PartitionSpec as P

LANES = 128
SUB = 8
BLOCK_ROWS = 64
ROWS_A = 32
W_ROWS = 8
GRID_BLOCK = 16
LOG2E = 1.4426950408889634
TWO_PI = 6.283185307179586
F32 = jnp.float32


def rows_of(array):
    own_cfg, width = array.shape
    rows = array.reshape(own_cfg, width // LANES, LANES).transpose(1, 0, 2)
    return rows.reshape(16, 4, BLOCK_ROWS, LANES)


def pack_kernel(mode, var, weight, part_a, b0, b1, b2, b3, w_vmem, sems, w_sem):
    lat = lax.axis_index("lat")
    rest = BLOCK_ROWS - ROWS_A
    copies = []
    for r, piece in enumerate((b0, b1, b2, b3)):
        other = jnp.bitwise_xor(lat, r)
        for a, array in enumerate((mode, var)):
            for src, dst in (
                (array.at[:, other, pl.ds(0, ROWS_A), :], part_a.at[pl.ds(16 * r, 16), pl.ds(a * ROWS_A, ROWS_A), :]),
                (array.at[:, other, pl.ds(ROWS_A, rest), :], piece.at[:, pl.ds(a * rest, rest), :]),
            ):
                copies.append(pltpu.make_async_copy(src, dst, sems.at[len(copies)]))
    for c in copies:
        c.start()
    w0 = jnp.full((64, W_ROWS // 2, LANES), weight[0], F32)
    w1 = jnp.full((64, W_ROWS // 2, LANES), weight[1], F32)
    w_vmem[...] = jnp.concatenate([w0, w1], axis=1)
    w_copy = pltpu.make_async_copy(w_vmem, part_a.at[:, pl.ds(2 * ROWS_A, W_ROWS), :], w_sem.at[0])
    w_copy.start()
    for c in copies:
        c.wait()
    w_copy.wait()


def pack(mode, var, weight):
    rest = BLOCK_ROWS - ROWS_A
    shape = jax.ShapeDtypeStruct
    return pl.pallas_call(
        pack_kernel,
        out_shape=(shape((64, 2 * ROWS_A + W_ROWS, LANES), F32),) + (shape((16, 2 * rest, LANES), F32),) * 4,
        in_specs=[pl.BlockSpec(memory_space=pl.ANY)] * 2 + [pl.BlockSpec(memory_space=pltpu.SMEM)],
        out_specs=[pl.BlockSpec(memory_space=pl.ANY)] * 5,
        scratch_shapes=[
            pltpu.VMEM((64, W_ROWS, LANES), F32),
            pltpu.SemaphoreType.DMA((16,)),
            pltpu.SemaphoreType.DMA((1,)),
        ],
        name="pack",
    )(mode, var, weight)


def merge_kernel(p0, p1, p2, p3, out, sems):
    lat = lax.axis_index("lat")
    copies = []
    for r, piece in enumerate((p0, p1, p2, p3)):
        start = 16 * jnp.bitwise_xor(lat, r)
        copies.append(pltpu.make_async_copy(piece, out.at[pl.ds(start, 16)], sems.at[r]))
    for c in copies:
        c.start()
    for c in copies:
        c.wait()


def merge(pieces):
    rows = pieces[0].shape[1]
    return pl.pallas_call(
        merge_kernel,
        out_shape=jax.ShapeDtypeStruct((64, rows, LANES), F32),
        in_specs=[pl.BlockSpec(memory_space=pl.ANY)] * 4,
        out_specs=pl.BlockSpec(memory_space=pl.ANY),
        scratch_shapes=[pltpu.SemaphoreType.DMA((4,))],
        name="merge",
    )(*pieces)


def tile_density(t, data, rows, norm, offset, modes, precs, logs, put):
    base = 2 * SUB * t

    def mode_of(c, k):
        return data[c, pl.ds(base + k, SUB, stride=2), :]

    def var_of(c, k):
        return data[c, pl.ds(rows + base + k, SUB, stride=2), :]

    def weight_of(c, k):
        return norm[pl.ds(2 * c + k, SUB, stride=0), :]

    zero = jnp.zeros((SUB, LANES), F32)

    def centre_step(i, sums):
        new = []
        for u in range(4):
            c = 4 * i + u
            for k in range(2):
                m = mode_of(c, k)
                modes[2 * c + k] = m
                new.append(weight_of(c, k) * m)
        return tuple(s + (new[2 * n] + new[2 * n + 1]) for n, s in enumerate(sums))

    s = lax.fori_loop(0, 16, centre_step, (zero,) * 4)
    centre = (s[0] + s[1]) + (s[2] + s[3])

    def spread_step(i, sums):
        new = []
        for u in range(4):
            c = 4 * i + u
            for k in range(2):
                v = var_of(c, k)
                w = weight_of(c, k)
                d = modes[2 * c + k] - centre
                new.append(w * (v + d * d))
                inverse = 1.0 / v
                precs[2 * c + k] = (-0.5 * LOG2E) * inverse
                logs[2 * c + k] = 0.5 * jnp.log2((w * w) * (1.0 / TWO_PI) * inverse)
        return tuple(s + (new[2 * n] + new[2 * n + 1]) for n, s in enumerate(sums))

    s = lax.fori_loop(0, 16, spread_step, (zero,) * 4)
    spread = jnp.sqrt((s[0] + s[1]) + (s[2] + s[3]))

    def grid_block(b, _):
        points = [centre + offset[GRID_BLOCK * b + g] * spread for g in range(GRID_BLOCK)]

        def config_step(k, sums):
            m, p, lc = modes[k], precs[k], logs[k]
            out = []
            for g in range(GRID_BLOCK):
                gap = points[g] - m
                out.append(sums[g] + jnp.exp2(lc + p * (gap * gap)))
            return tuple(out)

        sums = lax.fori_loop(0, 128, config_step, (zero,) * GRID_BLOCK, unroll=2)
        for g in range(GRID_BLOCK):
            put(t, GRID_BLOCK * b + g, sums[g] * spread)
        return 0

    lax.fori_loop(0, 64 // GRID_BLOCK, grid_block, 0)
    return centre, spread


def first_kernel(data, offset, out, norm, modes, precs, logs):
    groups = ROWS_A // 2
    rows = 2 * ROWS_A
    total = jnp.zeros((SUB, LANES), F32)
    for c in range(64):
        for k in range(2):
            total = total + data[c, pl.ds(rows + k * (W_ROWS // 2), SUB, stride=0), :]
    inverse = 1.0 / total[0:1]
    for c in range(64):
        for k in range(2):
            row = rows + k * (W_ROWS // 2)
            norm[2 * c + k : 2 * c + k + 1, :] = data[c, row : row + 1, :] * inverse

    def put(t, g, value):
        out[pl.ds(SUB * 64 * t + g, SUB, stride=64), :] = value

    def tile(t, _):
        centre, spread = tile_density(t, data, ROWS_A, norm, offset, modes, precs, logs, put)
        out[pl.ds(pl.multiple_of(64 * groups + SUB * t, SUB), SUB), :] = centre
        out[pl.ds(pl.multiple_of(65 * groups + SUB * t, SUB), SUB), :] = spread
        return 0

    lax.fori_loop(0, groups // SUB, tile, 0)


def second_kernel(data, offset, norm, other, density, moments, held, modes, precs, logs):
    groups_a = ROWS_A // 2
    rest = BLOCK_ROWS - ROWS_A

    def put(t, g, value):
        held[pl.ds(g, SUB, stride=64), :] = value

    def tile(t, _):
        centre, spread = tile_density(t, data, rest, norm, offset, modes, precs, logs, put)
        for j in range(SUB):
            at = pl.ds(pl.multiple_of((groups_a + SUB * t + j) * LANES, LANES), LANES)
            density[:, at] = held[64 * j : 64 * (j + 1), :]
            moments[0:1, at] = centre[j : j + 1]
            moments[1:2, at] = spread[j : j + 1]
        return 0

    lax.fori_loop(0, rest // 2 // SUB, tile, 0)
    for j in range(groups_a):
        density[:, j * LANES : (j + 1) * LANES] = other[64 * j : 64 * (j + 1), :]
        moments[0:1, j * LANES : (j + 1) * LANES] = other[64 * groups_a + j : 64 * groups_a + j + 1, :]
        moments[1:2, j * LANES : (j + 1) * LANES] = other[65 * groups_a + j : 65 * groups_a + j + 1, :]


def scratch():
    return [pltpu.VMEM((128, SUB, LANES), F32)] * 3


def cost(groups):
    work = 128 * 64 * groups * LANES
    return pl.CostEstimate(flops=6 * work, transcendentals=work, bytes_accessed=4 * 128 * 2 * groups * LANES)


def first_density(data, offset):
    groups = ROWS_A // 2
    shape = jax.ShapeDtypeStruct
    return pl.pallas_call(
        first_kernel,
        out_shape=(shape((66 * groups, LANES), F32), shape((128, LANES), F32)),
        in_specs=[pl.BlockSpec(memory_space=pltpu.VMEM), pl.BlockSpec(memory_space=pltpu.SMEM)],
        out_specs=[pl.BlockSpec(memory_space=pltpu.VMEM)] * 2,
        scratch_shapes=scratch(),
        cost_estimate=cost(groups),
        name="first_density",
    )(data, offset)


def second_density(data, offset, norm, other):
    groups = (BLOCK_ROWS - ROWS_A) // 2
    width = BLOCK_ROWS // 2 * LANES
    shape = jax.ShapeDtypeStruct
    vmem = pl.BlockSpec(memory_space=pltpu.VMEM)
    return pl.pallas_call(
        second_kernel,
        out_shape=(shape((64, width), F32), shape((2, width), F32)),
        in_specs=[vmem, pl.BlockSpec(memory_space=pltpu.SMEM), vmem, vmem],
        out_specs=[vmem] * 2,
        scratch_shapes=[pltpu.VMEM((SUB * 64, LANES), F32)] + scratch(),
        cost_estimate=cost(groups),
        name="second_density",
    )(data, offset, norm, other)


def exchanged(parts):
    return lax.all_to_all(parts, "cfg", split_axis=0, concat_axis=0, tiled=True)


def per_device(latent_mode, latent_var, config_weight, grid_offset):
    part_a, *pieces = pack(rows_of(latent_mode), rows_of(latent_var), config_weight)
    with jax.named_scope("xa"):
        data_a = exchanged(part_a)
    arrived = [pieces[0]]
    for r in range(1, 4):
        with jax.named_scope(f"lat{r}"):
            arrived.append(lax.ppermute(pieces[r], "lat", [(l, l ^ r) for l in range(4)]))
    with jax.named_scope("merge"):
        part_b = merge(arrived)
    with jax.named_scope("xb"):
        data_b = exchanged(part_b)
    with jax.named_scope("da"):
        sums_a, norm = first_density(data_a, grid_offset)
    home = [
        ((16 * z + c) * 4 + l, (16 * l + c) * 4 + (z ^ l)) for z in range(4) for c in range(16) for l in range(4)
    ]
    with jax.named_scope("home"):
        sums_a = lax.ppermute(sums_a, ("cfg", "lat"), home)
    with jax.named_scope("db"):
        density, moments = second_density(data_b, grid_offset, norm, sums_a)
    return (density, moments)


def solution(mesh):
    return jax.shard_map(
        per_device,
        mesh=mesh,
        in_specs=(P("cfg", "lat"), P("cfg", "lat"), P("cfg"), P()),
        out_specs=(P(None, ("cfg", "lat")), P(None, ("cfg", "lat"))),
        check_vma=False,
    )
```

```python
import jax
import jax.numpy as jnp
from jax import lax
from jax.experimental import pallas as pl
from jax.experimental.pallas import tpu as pltpu
from jax.sharding import PartitionSpec as P

LANES = 128
SUB = 8
BLOCK_ROWS = 64
ROWS_A = 32
W_ROWS = 8
GRID_BLOCK = 16
UNROLL = 8
LOG2E = 1.4426950408889634
TWO_PI = 6.283185307179586
F32 = jnp.float32


def rows_of(array):
    own_cfg, width = array.shape
    rows = array.reshape(own_cfg, width // LANES, LANES).transpose(1, 0, 2)
    return rows.reshape(16, 4, BLOCK_ROWS, LANES)


def pack_kernel(mode, var, weight, part_a, b0, b1, b2, b3, sems):
    lat = lax.axis_index("lat")
    rest = BLOCK_ROWS - ROWS_A
    copies = []
    for r, piece in enumerate((b0, b1, b2, b3)):
        other = jnp.bitwise_xor(lat, r)
        for a, array in enumerate((mode, var)):
            for src, dst in (
                (array.at[:, other, pl.ds(0, ROWS_A), :], part_a.at[pl.ds(16 * r, 16), pl.ds(a * ROWS_A, ROWS_A), :]),
                (array.at[:, other, pl.ds(ROWS_A, rest), :], piece.at[:, pl.ds(a * rest, rest), :]),
            ):
                copies.append(pltpu.make_async_copy(src, dst, sems.at[len(copies)]))
    for c in copies:
        c.start()
    for k in range(2):
        rows = pl.ds(2 * ROWS_A + k * (W_ROWS // 2), W_ROWS // 2)
        part_a[:, rows, :] = jnp.full((64, W_ROWS // 2, LANES), weight[k], F32)
    for c in copies:
        c.wait()


def pack(mode, var, weight):
    rest = BLOCK_ROWS - ROWS_A
    shape = jax.ShapeDtypeStruct
    return pl.pallas_call(
        pack_kernel,
        out_shape=(shape((64, 2 * ROWS_A + W_ROWS, LANES), F32),) + (shape((16, 2 * rest, LANES), F32),) * 4,
        in_specs=[pl.BlockSpec(memory_space=pl.ANY)] * 2 + [pl.BlockSpec(memory_space=pltpu.SMEM)],
        out_specs=[pl.BlockSpec(memory_space=pltpu.VMEM)] * 5,
        scratch_shapes=[pltpu.SemaphoreType.DMA((16,))],
        name="pack",
    )(mode, var, weight)


def merge_kernel(p0, p1, p2, p3, out):
    lat = lax.axis_index("lat")
    for r, piece in enumerate((p0, p1, p2, p3)):
        out[pl.ds(16 * jnp.bitwise_xor(lat, r), 16)] = piece[...]


def merge(pieces):
    rows = pieces[0].shape[1]
    vmem = pl.BlockSpec(memory_space=pltpu.VMEM)
    return pl.pallas_call(
        merge_kernel,
        out_shape=jax.ShapeDtypeStruct((64, rows, LANES), F32),
        in_specs=[vmem] * 4,
        out_specs=vmem,
        name="merge",
    )(*pieces)


def tile_density(t, data, rows, norm, offset, modes, precs, logs, put):
    base = 2 * SUB * t

    def mode_of(c, k):
        return data[c, pl.ds(base + k, SUB, stride=2), :]

    def var_of(c, k):
        return data[c, pl.ds(rows + base + k, SUB, stride=2), :]

    def weight_of(c, k):
        return norm[pl.ds(2 * c + k, SUB, stride=0), :]

    zero = jnp.zeros((SUB, LANES), F32)

    def centre_step(i, sums):
        new = []
        for u in range(4):
            c = 4 * i + u
            for k in range(2):
                m = mode_of(c, k)
                modes[2 * c + k] = m
                new.append(weight_of(c, k) * m)
        return tuple(s + (new[2 * n] + new[2 * n + 1]) for n, s in enumerate(sums))

    s = lax.fori_loop(0, 16, centre_step, (zero,) * 4)
    centre = (s[0] + s[1]) + (s[2] + s[3])

    def spread_step(i, sums):
        new = []
        for u in range(4):
            c = 4 * i + u
            for k in range(2):
                v = var_of(c, k)
                w = weight_of(c, k)
                d = modes[2 * c + k] - centre
                new.append(w * (v + d * d))
                inverse = 1.0 / v
                precs[2 * c + k] = (-0.5 * LOG2E) * inverse
                logs[2 * c + k] = 0.5 * jnp.log2((w * w) * (1.0 / TWO_PI) * inverse)
        return tuple(s + (new[2 * n] + new[2 * n + 1]) for n, s in enumerate(sums))

    s = lax.fori_loop(0, 16, spread_step, (zero,) * 4)
    spread = jnp.sqrt((s[0] + s[1]) + (s[2] + s[3]))

    def grid_block(b, _):
        points = [centre + offset[GRID_BLOCK * b + g] * spread for g in range(GRID_BLOCK)]

        def config_step(k, sums):
            m, p, lc = modes[k], precs[k], logs[k]
            out = []
            for g in range(GRID_BLOCK):
                gap = points[g] - m
                out.append(sums[g] + jnp.exp2(lc + p * (gap * gap)))
            return tuple(out)

        sums = lax.fori_loop(0, 128, config_step, (zero,) * GRID_BLOCK, unroll=UNROLL)
        for g in range(GRID_BLOCK):
            put(t, GRID_BLOCK * b + g, sums[g] * spread)
        return 0

    lax.fori_loop(0, 64 // GRID_BLOCK, grid_block, 0)
    return centre, spread


def norm_kernel_rows(data, norm):
    rows = 2 * ROWS_A
    total = jnp.zeros((SUB, LANES), F32)
    for c in range(64):
        for k in range(2):
            total = total + data[c, pl.ds(rows + k * (W_ROWS // 2), SUB, stride=0), :]
    inverse = 1.0 / total[0:1]
    for c in range(64):
        for k in range(2):
            row = rows + k * (W_ROWS // 2)
            norm[2 * c + k : 2 * c + k + 1, :] = data[c, row : row + 1, :] * inverse


def part_sums(rows, data, offset, norm, out, modes, precs, logs):
    groups = rows // 2

    def put(t, g, value):
        out[pl.ds(SUB * 64 * t + g, SUB, stride=64), :] = value

    def tile(t, _):
        centre, spread = tile_density(t, data, rows, norm, offset, modes, precs, logs, put)
        out[pl.ds(pl.multiple_of(64 * groups + SUB * t, SUB), SUB), :] = centre
        out[pl.ds(pl.multiple_of(65 * groups + SUB * t, SUB), SUB), :] = spread
        return 0

    lax.fori_loop(0, groups // SUB, tile, 0)


def first_kernel(data, offset, out, norm, modes, precs, logs):
    norm_kernel_rows(data, norm)
    part_sums(ROWS_A, data, offset, norm, out, modes, precs, logs)


def second_kernel(data, offset, norm, out, modes, precs, logs):
    part_sums(BLOCK_ROWS - ROWS_A, data, offset, norm, out, modes, precs, logs)


def place_kernel(first, second, density, moments):
    start = 0
    for part in (first, second):
        groups = part.shape[0] // 66
        for j in range(groups):
            at = slice((start + j) * LANES, (start + j + 1) * LANES)
            density[:, at] = part[64 * j : 64 * (j + 1), :]
            moments[0:1, at] = part[64 * groups + j : 64 * groups + j + 1, :]
            moments[1:2, at] = part[65 * groups + j : 65 * groups + j + 1, :]
        start += groups


VMEM = pl.BlockSpec(memory_space=pltpu.VMEM)
SMEM = pl.BlockSpec(memory_space=pltpu.SMEM)


def scratch():
    return [pltpu.VMEM((128, SUB, LANES), F32)] * 3


def cost(groups):
    work = 128 * 64 * groups * LANES
    return pl.CostEstimate(flops=6 * work, transcendentals=work, bytes_accessed=4 * 128 * 2 * groups * LANES)


def first_density(data, offset):
    groups = ROWS_A // 2
    shape = jax.ShapeDtypeStruct
    return pl.pallas_call(
        first_kernel,
        out_shape=(shape((66 * groups, LANES), F32), shape((128, LANES), F32)),
        in_specs=[VMEM, SMEM],
        out_specs=[VMEM] * 2,
        scratch_shapes=scratch(),
        cost_estimate=cost(groups),
        name="first_density",
    )(data, offset)


def second_density(data, offset, norm):
    groups = (BLOCK_ROWS - ROWS_A) // 2
    return pl.pallas_call(
        second_kernel,
        out_shape=jax.ShapeDtypeStruct((66 * groups, LANES), F32),
        in_specs=[VMEM, SMEM, VMEM],
        out_specs=VMEM,
        scratch_shapes=scratch(),
        cost_estimate=cost(groups),
        name="second_density",
    )(data, offset, norm)


def place(first, second):
    width = BLOCK_ROWS // 2 * LANES
    shape = jax.ShapeDtypeStruct
    return pl.pallas_call(
        place_kernel,
        out_shape=(shape((64, width), F32), shape((2, width), F32)),
        in_specs=[VMEM] * 2,
        out_specs=[VMEM] * 2,
        name="place",
    )(first, second)


def exchanged(parts):
    return lax.all_to_all(parts, "cfg", split_axis=0, concat_axis=0, tiled=True)


def per_device(latent_mode, latent_var, config_weight, grid_offset):
    part_a, *pieces = pack(rows_of(latent_mode), rows_of(latent_var), config_weight)
    with jax.named_scope("xa"):
        data_a = exchanged(part_a)
    arrived = [pieces[0]]
    for r in range(1, 4):
        with jax.named_scope(f"lat{r}"):
            arrived.append(lax.ppermute(pieces[r], "lat", [(l, l ^ r) for l in range(4)]))
    with jax.named_scope("merge"):
        part_b = merge(arrived)
    with jax.named_scope("xb"):
        data_b = exchanged(part_b)
    with jax.named_scope("da"):
        sums_a, norm = first_density(data_a, grid_offset)
    home = [
        ((16 * z + c) * 4 + l, (16 * l + c) * 4 + (z ^ l)) for z in range(4) for c in range(16) for l in range(4)
    ]
    with jax.named_scope("home"):
        sums_a = lax.ppermute(sums_a, ("cfg", "lat"), home)
    with jax.named_scope("db"):
        sums_b = second_density(data_b, grid_offset, norm)
    with jax.named_scope("place"):
        density, moments = place(sums_a, sums_b)
    return (density, moments)


def solution(mesh):
    return jax.shard_map(
        per_device,
        mesh=mesh,
        in_specs=(P("cfg", "lat"), P("cfg", "lat"), P("cfg"), P()),
        out_specs=(P(None, ("cfg", "lat")), P(None, ("cfg", "lat"))),
        check_vma=False,
    )
```

```python
import jax
import jax.numpy as jnp
from jax import lax
from jax.experimental import pallas as pl
from jax.experimental.pallas import tpu as pltpu
from jax.sharding import PartitionSpec as P

LANES = 128
SUB = 8
BLOCK_ROWS = 64
ROWS_A = 32
PITCH_A = 2 * ROWS_A + 1
GRID_BLOCK = 16
UNROLL = 16
LOG2E = 1.4426950408889634
TWO_PI = 6.283185307179586
F32 = jnp.float32
VMEM = pl.BlockSpec(memory_space=pltpu.VMEM)
SMEM = pl.BlockSpec(memory_space=pltpu.SMEM)


def rows_of(array):
    own_cfg, width = array.shape
    rows = array.reshape(own_cfg, width // LANES, LANES).transpose(1, 0, 2)
    return rows.reshape(16, 4, BLOCK_ROWS, LANES)


def held_at(z, lat):
    d = (lat - z) & 3
    return 2 * (d & 1) + (d >> 1)


def pack_first_kernel(mode, var, weight, out, sems):
    lat = lax.axis_index("lat")
    copies = []
    for z in range(4):
        for a, array in enumerate((mode, var)):
            src = array.at[:, held_at(z, lat), pl.ds(0, ROWS_A)]
            dst = out.at[pl.ds(16 * z, 16), pl.ds(a * ROWS_A, ROWS_A)]
            copies.append(pltpu.make_async_copy(src, dst, sems.at[len(copies)]))
    for c in copies:
        c.start()
    lane = lax.broadcasted_iota(jnp.int32, (1, LANES), 1)
    row = jnp.where(lane < LANES // 2, jnp.full((1, LANES), weight[0], F32), jnp.full((1, LANES), weight[1], F32))
    for c in range(64):
        out[c, 2 * ROWS_A] = row
    for c in copies:
        c.wait()


def pack_first(mode, var, weight):
    return pl.pallas_call(
        pack_first_kernel,
        out_shape=jax.ShapeDtypeStruct((64, PITCH_A, 1, LANES), F32),
        in_specs=[pl.BlockSpec(memory_space=pl.ANY)] * 2 + [SMEM],
        out_specs=VMEM,
        scratch_shapes=[pltpu.SemaphoreType.DMA((8,))],
        name="pack_first",
    )(mode[:, :, :, None, :], var[:, :, :, None, :], weight)


def pack_second_kernel(mode, var, b0, b1, b2, b3, sems):
    lat = lax.axis_index("lat")
    rest = BLOCK_ROWS - ROWS_A
    copies = []
    for r, piece in enumerate((b0, b1, b2, b3)):
        for a, array in enumerate((mode, var)):
            src = array.at[:, jnp.bitwise_xor(lat, r), pl.ds(ROWS_A, rest), :]
            copies.append(pltpu.make_async_copy(src, piece.at[:, pl.ds(a * rest, rest), :], sems.at[len(copies)]))
    for c in copies:
        c.start()
    for c in copies:
        c.wait()


def pack_second(mode, var):
    rest = BLOCK_ROWS - ROWS_A
    return pl.pallas_call(
        pack_second_kernel,
        out_shape=(jax.ShapeDtypeStruct((16, 2 * rest, LANES), F32),) * 4,
        in_specs=[pl.BlockSpec(memory_space=pl.ANY)] * 2,
        out_specs=[VMEM] * 4,
        scratch_shapes=[pltpu.SemaphoreType.DMA((8,))],
        name="pack_second",
    )(mode, var)


def merge_kernel(p0, p1, p2, p3, out):
    lat = lax.axis_index("lat")
    for r, piece in enumerate((p0, p1, p2, p3)):
        out[pl.ds(16 * jnp.bitwise_xor(lat, r), 16)] = piece[...]


def merge(pieces):
    rows = pieces[0].shape[1]
    return pl.pallas_call(
        merge_kernel,
        out_shape=jax.ShapeDtypeStruct((64, rows, LANES), F32),
        in_specs=[VMEM] * 4,
        out_specs=VMEM,
        name="merge",
    )(*pieces)


def tile_density(t, data, pitch, rows, norm, offset, modes, precs, logs, put):
    base = 2 * SUB * t

    def mode_of(c, k):
        return data[pl.ds(pitch * c + base + k, SUB, stride=2), :]

    def var_of(c, k):
        return data[pl.ds(pitch * c + rows + base + k, SUB, stride=2), :]

    def weight_of(c, k):
        return norm[pl.ds(2 * c + k, SUB, stride=0), :]

    zero = jnp.zeros((SUB, LANES), F32)

    def centre_step(i, sums):
        new = []
        for u in range(4):
            c = 4 * i + u
            for k in range(2):
                m = mode_of(c, k)
                modes[2 * c + k] = m
                new.append(weight_of(c, k) * m)
        return tuple(s + (new[2 * n] + new[2 * n + 1]) for n, s in enumerate(sums))

    s = lax.fori_loop(0, 16, centre_step, (zero,) * 4)
    centre = (s[0] + s[1]) + (s[2] + s[3])

    def spread_step(i, sums):
        new = []
        for u in range(4):
            c = 4 * i + u
            for k in range(2):
                v = var_of(c, k)
                w = weight_of(c, k)
                d = modes[2 * c + k] - centre
                new.append(w * (v + d * d))
                inverse = 1.0 / v
                precs[2 * c + k] = (-0.5 * LOG2E) * inverse
                logs[2 * c + k] = 0.5 * jnp.log2((w * w) * (1.0 / TWO_PI) * inverse)
        return tuple(s + (new[2 * n] + new[2 * n + 1]) for n, s in enumerate(sums))

    s = lax.fori_loop(0, 16, spread_step, (zero,) * 4)
    spread = jnp.sqrt((s[0] + s[1]) + (s[2] + s[3]))

    def grid_block(b, _):
        points = [centre + offset[GRID_BLOCK * b + g] * spread for g in range(GRID_BLOCK)]

        def config_step(k, sums):
            m, p, lc = modes[k], precs[k], logs[k]
            out = []
            for g in range(GRID_BLOCK):
                gap = points[g] - m
                out.append(sums[g] + jnp.exp2(lc + p * (gap * gap)))
            return tuple(out)

        sums = lax.fori_loop(0, 128, config_step, (zero,) * GRID_BLOCK, unroll=UNROLL)
        for g in range(GRID_BLOCK):
            put(t, GRID_BLOCK * b + g, sums[g] * spread)
        return 0

    lax.fori_loop(0, 64 // GRID_BLOCK, grid_block, 0)
    return centre, spread


def normalise(data, norm):
    lane = lax.broadcasted_iota(jnp.int32, (1, LANES), 1)
    rows = [data[PITCH_A * c + 2 * ROWS_A : PITCH_A * c + 2 * ROWS_A + 1, :] for c in range(64)]
    rows = [(jnp.where(lane < 1, r, 0.0), jnp.where(lane == LANES - 1, r, 0.0)) for r in rows]
    rows = [jnp.sum(r, axis=1, keepdims=True) for pair in rows for r in pair]
    total = rows
    while len(total) > 1:
        total = [a + b for a, b in zip(total[::2], total[1::2])]
    inverse = 1.0 / total[0]
    for k, r in enumerate(rows):
        norm[k : k + 1, :] = jnp.broadcast_to(r * inverse, (1, LANES))


def part_sums(pitch, rows, data, offset, norm, out, modes, precs, logs):
    groups = rows // 2

    def put(t, g, value):
        out[pl.ds(SUB * 64 * t + g, SUB, stride=64), :] = value

    def tile(t, _):
        centre, spread = tile_density(t, data, pitch, rows, norm, offset, modes, precs, logs, put)
        out[pl.ds(pl.multiple_of(64 * groups + SUB * t, SUB), SUB), :] = centre
        out[pl.ds(pl.multiple_of(65 * groups + SUB * t, SUB), SUB), :] = spread
        return 0

    lax.fori_loop(0, groups // SUB, tile, 0)


def first_kernel(data, offset, out, norm, modes, precs, logs):
    normalise(data, norm)
    part_sums(PITCH_A, ROWS_A, data, offset, norm, out, modes, precs, logs)


def second_kernel(data, offset, norm, out, modes, precs, logs):
    rest = BLOCK_ROWS - ROWS_A
    part_sums(2 * rest, rest, data, offset, norm, out, modes, precs, logs)


def place_kernel(first, second, density, moments):
    start = 0
    for part in (first, second):
        groups = part.shape[0] // 66
        for j in range(groups):
            at = slice((start + j) * LANES, (start + j + 1) * LANES)
            density[:, at] = part[64 * j : 64 * (j + 1), :]
            moments[0:1, at] = part[64 * groups + j : 64 * groups + j + 1, :]
            moments[1:2, at] = part[65 * groups + j : 65 * groups + j + 1, :]
        start += groups


def scratch():
    return [pltpu.VMEM((128, SUB, LANES), F32)] * 3


def cost(groups):
    work = 128 * 64 * groups * LANES
    return pl.CostEstimate(flops=6 * work, transcendentals=work, bytes_accessed=4 * 128 * 2 * groups * LANES)


def first_density(data, offset):
    groups = ROWS_A // 2
    shape = jax.ShapeDtypeStruct
    return pl.pallas_call(
        first_kernel,
        out_shape=(shape((66 * groups, LANES), F32), shape((128, LANES), F32)),
        in_specs=[VMEM, SMEM],
        out_specs=[VMEM] * 2,
        scratch_shapes=scratch(),
        cost_estimate=cost(groups),
        name="first_density",
    )(data, offset)


def second_density(data, offset, norm):
    groups = (BLOCK_ROWS - ROWS_A) // 2
    return pl.pallas_call(
        second_kernel,
        out_shape=jax.ShapeDtypeStruct((66 * groups, LANES), F32),
        in_specs=[VMEM, SMEM, VMEM],
        out_specs=VMEM,
        scratch_shapes=scratch(),
        cost_estimate=cost(groups),
        name="second_density",
    )(data, offset, norm)


def place(first, second):
    width = BLOCK_ROWS // 2 * LANES
    shape = jax.ShapeDtypeStruct
    return pl.pallas_call(
        place_kernel,
        out_shape=(shape((64, width), F32), shape((2, width), F32)),
        in_specs=[VMEM] * 2,
        out_specs=[VMEM] * 2,
        name="place",
    )(first, second)


def exchanged(parts):
    return lax.all_to_all(parts, "cfg", split_axis=0, concat_axis=0, tiled=True)


def per_device(latent_mode, latent_var, config_weight, grid_offset):
    mode, var = rows_of(latent_mode), rows_of(latent_var)
    part_a = pack_first(mode, var, config_weight)
    data_a = exchanged(part_a)
    pieces = pack_second(mode, var)
    arrived = [pieces[0]]
    for r in range(1, 4):
        arrived.append(lax.ppermute(pieces[r], "lat", [(l, l ^ r) for l in range(4)]))
    part_b = merge(arrived)
    data_b = exchanged(part_b)
    sums_a, norm = first_density(data_a.reshape(-1, LANES), grid_offset)
    each = [(z, c, l) for z in range(4) for c in range(16) for l in range(4)]
    along_x = [((16 * z + c) * 4 + l, (16 * z + c) * 4 + held_at(z, l)) for z, c, l in each]
    along_z = [((16 * z + c) * 4 + held_at(z, l), (16 * l + c) * 4 + held_at(z, l)) for z, c, l in each]
    sums_a = lax.ppermute(sums_a, ("cfg", "lat"), along_x)
    sums_a = lax.ppermute(sums_a, ("cfg", "lat"), along_z)
    sums_b = second_density(data_b.reshape(-1, LANES), grid_offset, norm)
    density, moments = place(sums_a, sums_b)
    return (density, moments)


def solution(mesh):
    return jax.shard_map(
        per_device,
        mesh=mesh,
        in_specs=(P("cfg", "lat"), P("cfg", "lat"), P("cfg"), P()),
        out_specs=(P(None, ("cfg", "lat")), P(None, ("cfg", "lat"))),
        check_vma=False,
    )
```

```python
import jax
import jax.numpy as jnp
from jax import lax
from jax.experimental import pallas as pl
from jax.experimental.pallas import tpu as pltpu
from jax.sharding import PartitionSpec as P


LANES = 128
SUB = 8
BLOCK_ROWS = 64
ROWS_A = 36
PITCH_A = 2 * ROWS_A + 1
UNROLL = 32
LOG2E = 1.4426950408889634
TWO_PI = 6.283185307179586
F32 = jnp.float32
VMEM = pl.BlockSpec(memory_space=pltpu.VMEM)
SMEM = pl.BlockSpec(memory_space=pltpu.SMEM)
HBM = pl.BlockSpec(memory_space=pl.ANY)


def rows_of(array):
    own_cfg, width = array.shape
    rows = array.reshape(own_cfg, width // LANES, LANES).transpose(1, 0, 2)
    return rows.reshape(16, 4, BLOCK_ROWS, LANES)


def held_at(z, lat):
    d = (lat - z) & 3
    return 2 * (d & 1) + (d >> 1)


def pack_first_kernel(mode, var, weight, out, held, in_sems, out_sems):
    lat = lax.axis_index("lat")
    arrive, leave = [], []
    for z in range(4):
        here = []
        for a, array in enumerate((mode, var)):
            src = array.at[:, held_at(z, lat), pl.ds(0, ROWS_A)]
            dst = held.at[pl.ds(16 * z, 16), pl.ds(a * ROWS_A, ROWS_A)]
            here.append(pltpu.make_async_copy(src, dst, in_sems.at[2 * z + a]))
        arrive.append(here)
        at = pl.ds(16 * z, 16)
        leave.append(pltpu.make_async_copy(held.at[at], out.at[at], out_sems.at[z]))
    for here in arrive:
        for c in here:
            c.start()
    lane = lax.broadcasted_iota(jnp.int32, (1, LANES), 1)
    row = jnp.where(lane < LANES // 2, jnp.full((1, LANES), weight[0], F32), jnp.full((1, LANES), weight[1], F32))
    for c in range(64):
        held[c, 2 * ROWS_A] = row
    for here, go in zip(arrive, leave):
        for c in here:
            c.wait()
        go.start()
    for go in leave:
        go.wait()


def pack_first(mode, var, weight):
    shape = (64, PITCH_A, 1, LANES)
    return pl.pallas_call(
        pack_first_kernel,
        out_shape=jax.ShapeDtypeStruct(shape, F32),
        in_specs=[HBM] * 2 + [SMEM],
        out_specs=HBM,
        scratch_shapes=[pltpu.VMEM(shape, F32), pltpu.SemaphoreType.DMA((8,)), pltpu.SemaphoreType.DMA((4,))],
        name="pack_first",
    )(mode[:, :, :, None, :], var[:, :, :, None, :], weight)


def pack_second_kernel(mode, var, b0, b1, b2, b3, h0, h1, h2, h3, in_sems, out_sems):
    lat = lax.axis_index("lat")
    rest = BLOCK_ROWS - ROWS_A
    arrive, leave = [], []
    for r, piece, held in ((3, b3, h3), (2, b2, h2), (1, b1, h1), (0, b0, h0)):
        here = []
        for a, array in enumerate((mode, var)):
            src = array.at[:, jnp.bitwise_xor(lat, r), pl.ds(ROWS_A, rest)]
            here.append(pltpu.make_async_copy(src, held.at[:, pl.ds(a * rest, rest)], in_sems.at[2 * r + a]))
        arrive.append(here)
        leave.append(pltpu.make_async_copy(held, piece, out_sems.at[r]))
    for here in arrive:
        for c in here:
            c.start()
    for here, go in zip(arrive, leave):
        for c in here:
            c.wait()
        go.start()
    for go in leave:
        go.wait()


def pack_second(mode, var):
    shape = (16, 2 * (BLOCK_ROWS - ROWS_A), 1, LANES)
    return pl.pallas_call(
        pack_second_kernel,
        out_shape=(jax.ShapeDtypeStruct(shape, F32),) * 4,
        in_specs=[HBM] * 2,
        out_specs=[HBM] * 4,
        scratch_shapes=[pltpu.VMEM(shape, F32)] * 4 + [pltpu.SemaphoreType.DMA((8,)), pltpu.SemaphoreType.DMA((4,))],
        name="pack_second",
    )(mode[:, :, :, None, :], var[:, :, :, None, :])


def merge_kernel(p0, p1, p2, p3, grid_offset, out, offset, held, in_sems, out_sems):
    lat = lax.axis_index("lat")
    arrive, leave = [], []
    for r, piece in enumerate((p0, p1, p2, p3)):
        at = pl.ds(16 * jnp.bitwise_xor(lat, r), 16)
        arrive.append(pltpu.make_async_copy(piece, held.at[r], in_sems.at[r]))
        leave.append(pltpu.make_async_copy(held.at[r], out.at[at], out_sems.at[r]))
    for c in arrive:
        c.start()
    for g in range(64):
        offset[g : g + 1, :] = jnp.full((1, LANES), grid_offset[g], F32)
    for c, go in zip(arrive, leave):
        c.wait()
        go.start()
    for go in leave:
        go.wait()


def merge(pieces, grid_offset):
    rows = pieces[0].shape[1]
    return pl.pallas_call(
        merge_kernel,
        out_shape=(jax.ShapeDtypeStruct((64, rows, 1, LANES), F32), jax.ShapeDtypeStruct((64, LANES), F32)),
        in_specs=[HBM] * 4 + [SMEM],
        out_specs=[HBM, VMEM],
        scratch_shapes=[
            pltpu.VMEM((4, 16, rows, 1, LANES), F32),
            pltpu.SemaphoreType.DMA((4,)),
            pltpu.SemaphoreType.DMA((4,)),
        ],
        name="merge",
    )(*pieces, grid_offset)


def prepare(rows, load, norm, modes, precs, logs, centres, spreads):
    groups = rows // 2
    zero = jnp.zeros((SUB, LANES), F32)
    for n, base in enumerate(starts_of(groups)):
        at = slice(SUB * n, SUB * (n + 1))

        def centre_step(i, sums, base=base, at=at):
            new = []
            for u in range(4):
                c = 4 * i + u
                for k in range(2):
                    m = load(c, 2 * base + k)
                    modes[2 * c + k, at, :] = m
                    new.append(norm[pl.ds(2 * c + k, SUB, stride=0), :] * m)
            return tuple(s + (new[2 * n] + new[2 * n + 1]) for n, s in enumerate(sums))

        s = lax.fori_loop(0, 16, centre_step, (zero,) * 4)
        centre = (s[0] + s[1]) + (s[2] + s[3])

        def spread_step(i, sums, base=base, at=at, centre=centre):
            new = []
            for u in range(4):
                c = 4 * i + u
                for k in range(2):
                    v = load(c, rows + 2 * base + k)
                    w = norm[pl.ds(2 * c + k, SUB, stride=0), :]
                    d = modes[2 * c + k, at, :] - centre
                    new.append(w * (v + d * d))
                    inverse = 1.0 / v
                    precs[2 * c + k, at, :] = (-0.5 * LOG2E) * inverse
                    logs[2 * c + k, at, :] = 0.5 * jnp.log2((w * w) * (1.0 / TWO_PI) * inverse)
            return tuple(s + (new[2 * n] + new[2 * n + 1]) for n, s in enumerate(sums))

        s = lax.fori_loop(0, 16, spread_step, (zero,) * 4)
        centres[at, :] = centre
        spreads[at, :] = jnp.sqrt((s[0] + s[1]) + (s[2] + s[3]))


def starts_of(groups):
    return [min(SUB * n, groups - SUB) for n in range(-(-groups // SUB))]


def row_of(group, groups):
    last = groups - groups % SUB
    return group if last == groups else jnp.where(group < last, group, group + SUB - groups % SUB)


def densities(groups, offset, modes, precs, logs, centres, spreads, put, done=lambda q: None):
    def pair(q, _):
        rows = [row_of(2 * q + n, groups) for n in range(2)]
        spread = [spreads[pl.ds(r, SUB, stride=0), :] for r in rows]
        centre = [centres[pl.ds(r, SUB, stride=0), :] for r in rows]
        points = [[c + offset[SUB * b : SUB * (b + 1), :] * s for b in range(8)] for c, s in zip(centre, spread)]

        def config_step(k, sums):
            out = []
            for n, r in enumerate(rows):
                m, p, lc = (ref[k, pl.ds(r, SUB, stride=0), :] for ref in (modes, precs, logs))
                for b in range(8):
                    gap = points[n][b] - m
                    out.append(sums[8 * n + b] + jnp.exp2(lc + p * (gap * gap)))
            return tuple(out)

        sums = lax.fori_loop(0, 128, config_step, (jnp.zeros((SUB, LANES), F32),) * 16, unroll=UNROLL)
        for n in range(2):
            put(2 * q + n, [sums[8 * n + b] * spread[n] for b in range(8)])
        done(q)
        return 0

    lax.fori_loop(0, groups // 2, pair, 0)


def normalise(data, norm):
    lane = lax.broadcasted_iota(jnp.int32, (1, LANES), 1)
    rows = [data[PITCH_A * c + 2 * ROWS_A : PITCH_A * c + 2 * ROWS_A + 1, :] for c in range(64)]
    rows = [(jnp.where(lane < 1, r, 0.0), jnp.where(lane == LANES - 1, r, 0.0)) for r in rows]
    rows = [jnp.sum(r, axis=1, keepdims=True) for pair in rows for r in pair]
    total = rows
    while len(total) > 1:
        total = [a + b for a, b in zip(total[::2], total[1::2])]
    inverse = 1.0 / total[0]
    for k, r in enumerate(rows):
        norm[k : k + 1, :] = jnp.broadcast_to(r * inverse, (1, LANES))


def first_kernel(data, offset, out, norm, modes, precs, logs, centres, spreads):
    groups = ROWS_A // 2
    normalise(data, norm)

    def load(c, row):
        return data[pl.ds(PITCH_A * c + row, SUB, stride=2), :]

    prepare(ROWS_A, load, norm, modes, precs, logs, centres, spreads)

    def put(group, values):
        for b, value in enumerate(values):
            out[pl.ds(pl.multiple_of(64 * group + SUB * b, SUB), SUB), :] = value

    densities(groups, offset, modes, precs, logs, centres, spreads, put)
    for group in range(groups):
        row = group if group < groups - groups % SUB else group + SUB - groups % SUB
        out[64 * groups + group : 64 * groups + group + 1, :] = centres[row : row + 1, :]
        out[65 * groups + group : 65 * groups + group + 1, :] = spreads[row : row + 1, :]


def second_kernel(
    data, offset, norm, density, moments, modes, precs, logs, centres, spreads, own, own_moments, out_sems
):
    rows = BLOCK_ROWS - ROWS_A
    groups = rows // 2

    def load(c, row):
        return data[pl.ds(2 * rows * c + row, SUB, stride=2), :]

    prepare(rows, load, norm, modes, precs, logs, centres, spreads)
    for group in range(groups):
        row = group if group < groups - groups % SUB else group + SUB - groups % SUB
        own_moments[0:1, group * LANES : (group + 1) * LANES] = centres[row : row + 1, :]
        own_moments[1:2, group * LANES : (group + 1) * LANES] = spreads[row : row + 1, :]
    start = ROWS_A // 2 * LANES
    moments_copy = pltpu.make_async_copy(own_moments, moments.at[:, pl.ds(start, groups * LANES)], out_sems.at[groups // 2])
    moments_copy.start()

    def columns(q):
        at = pl.multiple_of(q * 2 * LANES, 2 * LANES)
        src = own.at[:, pl.ds(at, 2 * LANES)]
        dst = density.at[:, pl.ds(pl.multiple_of(start + at, 2 * LANES), 2 * LANES)]
        return pltpu.make_async_copy(src, dst, out_sems.at[q])

    def put(group, values):
        for b, value in enumerate(values):
            own[SUB * b : SUB * (b + 1), pl.ds(pl.multiple_of(group * LANES, LANES), LANES)] = value

    densities(groups, offset, modes, precs, logs, centres, spreads, put, lambda q: columns(q).start())
    for q in range(groups // 2):
        columns(q).wait()
    moments_copy.wait()


def place_kernel(first, density_in, moments_in, tick, density, moments, held, held_moments, sems):
    groups = ROWS_A // 2
    for j in range(groups):
        at = slice(j * LANES, (j + 1) * LANES)
        held[:, at] = first[64 * j : 64 * (j + 1), :]
        held_moments[0:1, at] = first[64 * groups + j : 64 * groups + j + 1, :]
        held_moments[1:2, at] = first[65 * groups + j : 65 * groups + j + 1, :]
    at = pl.ds(0, groups * LANES)
    copies = [
        pltpu.make_async_copy(held, density.at[:, at], sems.at[0]),
        pltpu.make_async_copy(held_moments, moments.at[:, at], sems.at[1]),
    ]
    for c in copies:
        c.start()
    for c in copies:
        c.wait()


def scratch(groups):
    held = SUB * len(starts_of(groups))
    return [pltpu.VMEM((128, held, LANES), F32)] * 3 + [pltpu.VMEM((held, LANES), F32)] * 2


def cost(groups):
    work = 128 * 64 * groups * LANES
    return pl.CostEstimate(flops=6 * work, transcendentals=work, bytes_accessed=4 * 128 * 2 * groups * LANES)


def first_density(data, offset):
    groups = ROWS_A // 2
    shape = jax.ShapeDtypeStruct
    return pl.pallas_call(
        first_kernel,
        out_shape=(shape((66 * groups, LANES), F32), shape((128, LANES), F32)),
        in_specs=[VMEM, VMEM],
        out_specs=[VMEM] * 2,
        scratch_shapes=scratch(groups),
        cost_estimate=cost(groups),
        name="first_density",
    )(data, offset)


def outputs():
    width = BLOCK_ROWS // 2 * LANES
    return (jax.ShapeDtypeStruct((64, width), F32), jax.ShapeDtypeStruct((2, width), F32))


def staged(groups):
    return [pltpu.VMEM((64, groups * LANES), F32), pltpu.VMEM((2, groups * LANES), F32)]


def second_density(data, offset, norm):
    groups = (BLOCK_ROWS - ROWS_A) // 2
    return pl.pallas_call(
        second_kernel,
        out_shape=outputs(),
        in_specs=[VMEM, VMEM, VMEM],
        out_specs=[HBM] * 2,
        scratch_shapes=scratch(groups)
        + staged(groups)
        + [
            pltpu.SemaphoreType.DMA((groups // 2 + 1,)),
        ],
        cost_estimate=cost(groups),
        name="second_density",
    )(data, offset, norm)


def place(first, density, moments, tick):
    return pl.pallas_call(
        place_kernel,
        out_shape=outputs(),
        in_specs=[VMEM, HBM, HBM, HBM],
        out_specs=[HBM] * 2,
        scratch_shapes=staged(ROWS_A // 2) + [pltpu.SemaphoreType.DMA((2,))],
        input_output_aliases={1: 0, 2: 1},
        name="place",
    )(first, density, moments, tick)


def in_vmem(array):
    return pltpu.with_memory_space_constraint(array, pltpu.VMEM)


def exchanged(parts):
    return lax.all_to_all(parts, "cfg", split_axis=0, concat_axis=0, tiled=True)


def way_home():
    along_x, along_z = [], []
    for z in range(4):
        for c in range(16):
            for l in range(4):
                lat = held_at(z, l)
                along_x.append(((16 * z + c) * 4 + l, (16 * z + c) * 4 + lat))
                along_z.append(((16 * z + c) * 4 + lat, (16 * l + c) * 4 + lat))
    return along_x, along_z


def per_device(latent_mode, latent_var, config_weight, grid_offset):
    mode, var = rows_of(latent_mode), rows_of(latent_var)
    part_a = pack_first(mode, var, config_weight)
    data_a = exchanged(part_a)
    pieces = pack_second(mode, var)
    arrived = [pieces[0]]
    for r in range(1, 4):
        arrived.append(lax.ppermute(pieces[r], "lat", [(l, l ^ r) for l in range(4)]))
    part_b, offset = merge(arrived, grid_offset)
    data_b = exchanged(part_b)
    sums_a, norm = first_density(in_vmem(data_a.reshape(-1, LANES)), offset)
    along_x, along_z = way_home()
    sums_a = lax.ppermute(sums_a, ("cfg", "lat"), along_x)
    tick = lax.ppermute(sums_a[:SUB], "lat", [(l, l ^ 1) for l in range(4)])
    sums_a = lax.ppermute(sums_a, ("cfg", "lat"), along_z)
    density, moments = second_density(in_vmem(data_b.reshape(-1, LANES)), offset, norm)
    density, moments = place(in_vmem(sums_a), density, moments, tick)
    return (density, moments)


def solution(mesh):
    return jax.shard_map(
        per_device,
        mesh=mesh,
        in_specs=(P("cfg", "lat"), P("cfg", "lat"), P("cfg"), P()),
        out_specs=(P(None, ("cfg", "lat")), P(None, ("cfg", "lat"))),
        check_vma=False,
    )
```

```python
import jax
import jax.numpy as jnp
from jax import lax
from jax.experimental import pallas as pl
from jax.experimental.pallas import tpu as pltpu
from jax.sharding import PartitionSpec as P


LANES = 128
SUB = 8
BLOCK_ROWS = 64
ROWS_A = 36
PITCH_A = 2 * ROWS_A + 1
UNROLL = 32
LOG2E = 1.4426950408889634
TWO_PI = 6.283185307179586
F32 = jnp.float32
VMEM = pl.BlockSpec(memory_space=pltpu.VMEM)
SMEM = pl.BlockSpec(memory_space=pltpu.SMEM)
HBM = pl.BlockSpec(memory_space=pl.ANY)


def rows_of(array):
    own_cfg, width = array.shape
    rows = array.reshape(own_cfg, width // LANES, LANES).transpose(1, 0, 2)
    return rows.reshape(16, 4, BLOCK_ROWS, LANES)


def held_at(z, lat):
    d = (lat - z) & 3
    return 2 * (d & 1) + (d >> 1)


def pack_first_kernel(mode, var, weight, out, held, in_sems, out_sems):
    lat = lax.axis_index("lat")
    arrive, leave = [], []
    for z in range(4):
        here = []
        for a, array in enumerate((mode, var)):
            src = array.at[:, held_at(z, lat), pl.ds(0, ROWS_A)]
            dst = held.at[pl.ds(16 * z, 16), pl.ds(a * ROWS_A, ROWS_A)]
            here.append(pltpu.make_async_copy(src, dst, in_sems.at[2 * z + a]))
        arrive.append(here)
        at = pl.ds(16 * z, 16)
        leave.append(pltpu.make_async_copy(held.at[at], out.at[at], out_sems.at[z]))
    for here in arrive:
        for c in here:
            c.start()
    lane = lax.broadcasted_iota(jnp.int32, (1, LANES), 1)
    row = jnp.where(lane < LANES // 2, jnp.full((1, LANES), weight[0], F32), jnp.full((1, LANES), weight[1], F32))
    for c in range(64):
        held[c, 2 * ROWS_A] = row
    for here, go in zip(arrive, leave):
        for c in here:
            c.wait()
        go.start()
    for go in leave:
        go.wait()


def pack_first(mode, var, weight):
    shape = (64, PITCH_A, 1, LANES)
    return pl.pallas_call(
        pack_first_kernel,
        out_shape=jax.ShapeDtypeStruct(shape, F32),
        in_specs=[HBM] * 2 + [SMEM],
        out_specs=HBM,
        scratch_shapes=[pltpu.VMEM(shape, F32), pltpu.SemaphoreType.DMA((8,)), pltpu.SemaphoreType.DMA((4,))],
        name="pack_first",
    )(mode[:, :, :, None, :], var[:, :, :, None, :], weight)


def pack_second_kernel(mode, var, b0, b1, b2, b3, h0, h1, h2, h3, in_sems, out_sems):
    lat = lax.axis_index("lat")
    rest = BLOCK_ROWS - ROWS_A
    arrive, leave = [], []
    for r, piece, held in ((3, b3, h3), (2, b2, h2), (1, b1, h1), (0, b0, h0)):
        here = []
        for a, array in enumerate((mode, var)):
            src = array.at[:, jnp.bitwise_xor(lat, r), pl.ds(ROWS_A, rest)]
            here.append(pltpu.make_async_copy(src, held.at[:, pl.ds(a * rest, rest)], in_sems.at[2 * r + a]))
        arrive.append(here)
        leave.append(pltpu.make_async_copy(held, piece, out_sems.at[r]))
    for here in arrive:
        for c in here:
            c.start()
    for here, go in zip(arrive, leave):
        for c in here:
            c.wait()
        go.start()
    for go in leave:
        go.wait()


def pack_second(mode, var):
    shape = (16, 2 * (BLOCK_ROWS - ROWS_A), 1, LANES)
    return pl.pallas_call(
        pack_second_kernel,
        out_shape=(jax.ShapeDtypeStruct(shape, F32),) * 4,
        in_specs=[HBM] * 2,
        out_specs=[HBM] * 4,
        scratch_shapes=[pltpu.VMEM(shape, F32)] * 4 + [pltpu.SemaphoreType.DMA((8,)), pltpu.SemaphoreType.DMA((4,))],
        name="pack_second",
    )(mode[:, :, :, None, :], var[:, :, :, None, :])


def merge_kernel(p0, p1, p2, p3, grid_offset, out, offset, held, in_sem, out_sems):
    lat = lax.axis_index("lat")
    arrive = pltpu.make_async_copy(p0, held, in_sem.at[0])
    arrive.start()
    leave = []
    for r, piece in enumerate((held, p1, p2, p3)):
        at = pl.ds(16 * jnp.bitwise_xor(lat, r), 16)
        leave.append(pltpu.make_async_copy(piece, out.at[at], out_sems.at[r]))
    for go in leave[1:]:
        go.start()
    for g in range(64):
        offset[g : g + 1, :] = jnp.full((1, LANES), grid_offset[g], F32)
    arrive.wait()
    leave[0].start()
    for go in leave:
        go.wait()


def merge(pieces, grid_offset):
    rows = pieces[0].shape[1]
    return pl.pallas_call(
        merge_kernel,
        out_shape=(jax.ShapeDtypeStruct((64, rows, 1, LANES), F32), jax.ShapeDtypeStruct((64, LANES), F32)),
        in_specs=[HBM] + [VMEM] * 3 + [SMEM],
        out_specs=[HBM, VMEM],
        scratch_shapes=[
            pltpu.VMEM((16, rows, 1, LANES), F32),
            pltpu.SemaphoreType.DMA((1,)),
            pltpu.SemaphoreType.DMA((4,)),
        ],
        name="merge",
    )(*pieces, grid_offset)


def prepare(rows, load, norm, modes, precs, logs, centres, spreads):
    groups = rows // 2
    zero = jnp.zeros((SUB, LANES), F32)
    for n, base in enumerate(starts_of(groups)):
        at = slice(SUB * n, SUB * (n + 1))

        def centre_step(i, sums, base=base, at=at):
            new = []
            for u in range(4):
                c = 4 * i + u
                for k in range(2):
                    m = load(c, 2 * base + k)
                    modes[2 * c + k, at, :] = m
                    new.append(norm[pl.ds(2 * c + k, SUB, stride=0), :] * m)
            return tuple(s + (new[2 * n] + new[2 * n + 1]) for n, s in enumerate(sums))

        s = lax.fori_loop(0, 16, centre_step, (zero,) * 4)
        centre = (s[0] + s[1]) + (s[2] + s[3])

        def spread_step(i, sums, base=base, at=at, centre=centre):
            new = []
            for u in range(4):
                c = 4 * i + u
                for k in range(2):
                    v = load(c, rows + 2 * base + k)
                    w = norm[pl.ds(2 * c + k, SUB, stride=0), :]
                    d = modes[2 * c + k, at, :] - centre
                    new.append(w * (v + d * d))
                    inverse = 1.0 / v
                    precs[2 * c + k, at, :] = (-0.5 * LOG2E) * inverse
                    logs[2 * c + k, at, :] = 0.5 * jnp.log2((w * w) * (1.0 / TWO_PI) * inverse)
            return tuple(s + (new[2 * n] + new[2 * n + 1]) for n, s in enumerate(sums))

        s = lax.fori_loop(0, 16, spread_step, (zero,) * 4)
        centres[at, :] = centre
        spreads[at, :] = jnp.sqrt((s[0] + s[1]) + (s[2] + s[3]))


def starts_of(groups):
    return [min(SUB * n, groups - SUB) for n in range(-(-groups // SUB))]


def row_of(group, groups):
    last = groups - groups % SUB
    return group if last == groups else jnp.where(group < last, group, group + SUB - groups % SUB)


def densities(groups, offset, modes, precs, logs, centres, spreads, put, done=lambda q: None):
    def pair(q, _):
        rows = [row_of(2 * q + n, groups) for n in range(2)]
        spread = [spreads[pl.ds(r, SUB, stride=0), :] for r in rows]
        centre = [centres[pl.ds(r, SUB, stride=0), :] for r in rows]
        points = [[c + offset[SUB * b : SUB * (b + 1), :] * s for b in range(8)] for c, s in zip(centre, spread)]

        def config_step(k, sums):
            out = []
            for n, r in enumerate(rows):
                m, p, lc = (ref[k, pl.ds(r, SUB, stride=0), :] for ref in (modes, precs, logs))
                for b in range(8):
                    gap = points[n][b] - m
                    out.append(sums[8 * n + b] + jnp.exp2(lc + p * (gap * gap)))
            return tuple(out)

        sums = lax.fori_loop(0, 128, config_step, (jnp.zeros((SUB, LANES), F32),) * 16, unroll=UNROLL)
        for n in range(2):
            put(2 * q + n, [sums[8 * n + b] * spread[n] for b in range(8)])
        done(q)
        return 0

    lax.fori_loop(0, groups // 2, pair, 0)


def normalise(data, norm):
    lane = lax.broadcasted_iota(jnp.int32, (1, LANES), 1)
    rows = [data[PITCH_A * c + 2 * ROWS_A : PITCH_A * c + 2 * ROWS_A + 1, :] for c in range(64)]
    rows = [(jnp.where(lane < 1, r, 0.0), jnp.where(lane == LANES - 1, r, 0.0)) for r in rows]
    rows = [jnp.sum(r, axis=1, keepdims=True) for pair in rows for r in pair]
    total = rows
    while len(total) > 1:
        total = [a + b for a, b in zip(total[::2], total[1::2])]
    inverse = 1.0 / total[0]
    for k, r in enumerate(rows):
        norm[k : k + 1, :] = jnp.broadcast_to(r * inverse, (1, LANES))


def first_kernel(data, offset, out, norm, modes, precs, logs, centres, spreads):
    groups = ROWS_A // 2
    normalise(data, norm)

    def load(c, row):
        return data[pl.ds(PITCH_A * c + row, SUB, stride=2), :]

    prepare(ROWS_A, load, norm, modes, precs, logs, centres, spreads)

    def put(group, values):
        for b, value in enumerate(values):
            out[pl.ds(pl.multiple_of(64 * group + SUB * b, SUB), SUB), :] = value

    densities(groups, offset, modes, precs, logs, centres, spreads, put)
    for group in range(groups):
        row = group if group < groups - groups % SUB else group + SUB - groups % SUB
        out[64 * groups + group : 64 * groups + group + 1, :] = centres[row : row + 1, :]
        out[65 * groups + group : 65 * groups + group + 1, :] = spreads[row : row + 1, :]


def second_kernel(
    data, offset, norm, density, moments, modes, precs, logs, centres, spreads, own, own_moments, out_sems
):
    rows = BLOCK_ROWS - ROWS_A
    groups = rows // 2

    def load(c, row):
        return data[pl.ds(2 * rows * c + row, SUB, stride=2), :]

    prepare(rows, load, norm, modes, precs, logs, centres, spreads)
    for group in range(groups):
        row = group if group < groups - groups % SUB else group + SUB - groups % SUB
        own_moments[0:1, group * LANES : (group + 1) * LANES] = centres[row : row + 1, :]
        own_moments[1:2, group * LANES : (group + 1) * LANES] = spreads[row : row + 1, :]
    start = ROWS_A // 2 * LANES
    moments_copy = pltpu.make_async_copy(own_moments, moments.at[:, pl.ds(start, groups * LANES)], out_sems.at[groups // 2])
    moments_copy.start()

    def columns(q):
        at = pl.multiple_of(q * 2 * LANES, 2 * LANES)
        src = own.at[:, pl.ds(at, 2 * LANES)]
        dst = density.at[:, pl.ds(pl.multiple_of(start + at, 2 * LANES), 2 * LANES)]
        return pltpu.make_async_copy(src, dst, out_sems.at[q])

    def put(group, values):
        for b, value in enumerate(values):
            own[SUB * b : SUB * (b + 1), pl.ds(pl.multiple_of(group * LANES, LANES), LANES)] = value

    densities(groups, offset, modes, precs, logs, centres, spreads, put, lambda q: columns(q).start())
    for q in range(groups // 2):
        columns(q).wait()
    moments_copy.wait()


def place_kernel(first, density_in, moments_in, tick, density, moments, held, held_moments, sems):
    groups = ROWS_A // 2
    for j in range(groups):
        at = slice(j * LANES, (j + 1) * LANES)
        held[:, at] = first[64 * j : 64 * (j + 1), :]
        held_moments[0:1, at] = first[64 * groups + j : 64 * groups + j + 1, :]
        held_moments[1:2, at] = first[65 * groups + j : 65 * groups + j + 1, :]
    at = pl.ds(0, groups * LANES)
    copies = [
        pltpu.make_async_copy(held, density.at[:, at], sems.at[0]),
        pltpu.make_async_copy(held_moments, moments.at[:, at], sems.at[1]),
    ]
    for c in copies:
        c.start()
    for c in copies:
        c.wait()


def scratch(groups):
    held = SUB * len(starts_of(groups))
    return [pltpu.VMEM((128, held, LANES), F32)] * 3 + [pltpu.VMEM((held, LANES), F32)] * 2


def cost(groups):
    work = 128 * 64 * groups * LANES
    return pl.CostEstimate(flops=6 * work, transcendentals=work, bytes_accessed=4 * 128 * 2 * groups * LANES)


def first_density(data, offset):
    groups = ROWS_A // 2
    shape = jax.ShapeDtypeStruct
    return pl.pallas_call(
        first_kernel,
        out_shape=(shape((66 * groups, LANES), F32), shape((128, LANES), F32)),
        in_specs=[VMEM, VMEM],
        out_specs=[VMEM] * 2,
        scratch_shapes=scratch(groups),
        cost_estimate=cost(groups),
        name="first_density",
    )(data, offset)


def outputs():
    width = BLOCK_ROWS // 2 * LANES
    return (jax.ShapeDtypeStruct((64, width), F32), jax.ShapeDtypeStruct((2, width), F32))


def staged(groups):
    return [pltpu.VMEM((64, groups * LANES), F32), pltpu.VMEM((2, groups * LANES), F32)]


def second_density(data, offset, norm):
    groups = (BLOCK_ROWS - ROWS_A) // 2
    return pl.pallas_call(
        second_kernel,
        out_shape=outputs(),
        in_specs=[VMEM, VMEM, VMEM],
        out_specs=[HBM] * 2,
        scratch_shapes=scratch(groups)
        + staged(groups)
        + [
            pltpu.SemaphoreType.DMA((groups // 2 + 1,)),
        ],
        cost_estimate=cost(groups),
        name="second_density",
    )(data, offset, norm)


def place(first, density, moments, tick):
    return pl.pallas_call(
        place_kernel,
        out_shape=outputs(),
        in_specs=[VMEM, HBM, HBM, HBM],
        out_specs=[HBM] * 2,
        scratch_shapes=staged(ROWS_A // 2) + [pltpu.SemaphoreType.DMA((2,))],
        input_output_aliases={1: 0, 2: 1},
        name="place",
    )(first, density, moments, tick)


def in_vmem(array):
    return pltpu.with_memory_space_constraint(array, pltpu.VMEM)


def exchanged(parts):
    return lax.all_to_all(parts, "cfg", split_axis=0, concat_axis=0, tiled=True)


def way_home():
    along_x, along_z = [], []
    for z in range(4):
        for c in range(16):
            for l in range(4):
                lat = held_at(z, l)
                along_x.append(((16 * z + c) * 4 + l, (16 * z + c) * 4 + lat))
                along_z.append(((16 * z + c) * 4 + lat, (16 * l + c) * 4 + lat))
    return along_x, along_z


def per_device(latent_mode, latent_var, config_weight, grid_offset):
    mode, var = rows_of(latent_mode), rows_of(latent_var)
    part_a = pack_first(mode, var, config_weight)
    data_a = exchanged(part_a)
    pieces = pack_second(mode, var)
    arrived = [pieces[0]]
    for r in range(1, 4):
        arrived.append(lax.ppermute(pieces[r], "lat", [(l, l ^ r) for l in range(4)]))
    part_b, offset = merge([arrived[0]] + [in_vmem(a) for a in arrived[1:]], grid_offset)
    data_b = exchanged(part_b)
    sums_a, norm = first_density(in_vmem(data_a.reshape(-1, LANES)), offset)
    along_x, along_z = way_home()
    sums_a = lax.ppermute(sums_a, ("cfg", "lat"), along_x)
    tick = lax.ppermute(sums_a[:SUB], "lat", [(l, l ^ 1) for l in range(4)])
    sums_a = lax.ppermute(sums_a, ("cfg", "lat"), along_z)
    density, moments = second_density(in_vmem(data_b.reshape(-1, LANES)), offset, norm)
    density, moments = place(in_vmem(sums_a), density, moments, tick)
    return (density, moments)


def solution(mesh):
    return jax.shard_map(
        per_device,
        mesh=mesh,
        in_specs=(P("cfg", "lat"), P("cfg", "lat"), P("cfg"), P()),
        out_specs=(P(None, ("cfg", "lat")), P(None, ("cfg", "lat"))),
        check_vma=False,
    )
```
